32 devices in a mesh: dp: 8 (over z, y), owner: 4 (over x, core).
Axes of the slice: x: 2, y: 2, z: 4, core: 2. Of those that a mesh axis runs over, the one named last changes fastest.
Arguments:
- grads: float32 [8, 32, 512, 128], P('dp', None, 'owner'), may hold values from -21 to 21
- momentum: float32 [64, 512, 128], P('dp', 'owner'), may hold values from -30 to 30
- slot_matrix: int32 [64], replicated, may hold values from -1 to 31, as said below
Outputs:
- updates: bfloat16 [32, 512, 128], P(None, 'owner')
- momentum_out: float32 [64, 512, 128], P('dp', 'owner')
The draws below stay inside these ranges and needn't reach their ends.
Inputs may be any that keep to these rules, and one draw needn't show every extreme that they name: `slot_matrix`: entry s names the block held by slot s, or is -1 if slot s is empty; slots s with s // 8 == g belong to the owner group at index g of dp. Every one of the 32 blocks is held by exactly one slot, and some group, drawn from the seed, has all 8 slots filled.
All inputs are finite; a program needn't handle non-finite values.
Results may differ from the reference program's by a relative error of at most 0.038.
Values may be sent and summed in bfloat16 or wider, within the bound.
A program may use at most 64 MiB of HBM per device.

```python
import math
import jax
import jax.numpy as jnp
from jax import lax

C = 512
R = 128
SLOTS = 8
ITERS = 5
MATS = 32
TOTAL_SLOTS = 64
N_DP = 8


def shape_scales(key):
    key_cols, key_rows = jax.random.split(jax.random.fold_in(key, 11))
    columns = jnp.exp(jax.random.uniform(key_cols, (C,), jnp.float32, 0.0, math.log(10.0)))
    trend = 3.0 ** (jnp.arange(C, dtype=jnp.float32) / (C - 1))
    columns = columns * trend
    rows_scale = jnp.exp(jax.random.uniform(key_rows, (R,), jnp.float32, 0.0, math.log(10.0)))
    both = columns[:, None] * rows_scale[None, :]
    return both / jnp.max(both)


def draw_grads(key, part):
    scaled = shape_scales(key)
    key_rep = jax.random.fold_in(jax.random.fold_in(key, 23), 0)
    key_noise = jax.random.fold_in(jax.random.fold_in(key, 23), 2)
    replica = jnp.exp(jax.random.uniform(key_rep, (N_DP, MATS, 1, 1), jnp.float32, -1.2, 1.2))
    values = jnp.clip(jax.random.normal(key_noise, (N_DP, MATS, C, R), jnp.float32), -5.0, 5.0)
    return 6.0 * values * replica * scaled / math.sqrt(N_DP)


def draw_momentum(key, part):
    scaled = shape_scales(key)
    key_noise = jax.random.fold_in(key, 37)
    values = jnp.clip(jax.random.normal(key_noise, (TOTAL_SLOTS, C, R), jnp.float32), -5.0, 5.0)
    return 6.0 * values * scaled


def draw_slot_matrix(key, part):
    key_full, key_score, key_ids = jax.random.split(jax.random.fold_in(key, 53), 3)
    filled_group = jax.random.randint(key_full, (), 0, N_DP)
    positions = jnp.arange(TOTAL_SLOTS, dtype=jnp.int32)
    score = jax.random.permutation(key_score, TOTAL_SLOTS).astype(jnp.int32) + TOTAL_SLOTS
    score = jnp.where(positions // SLOTS == filled_group, positions % SLOTS, score)
    ordering = jnp.argsort(score, stable=True).astype(jnp.int32)
    identity = jax.random.permutation(key_ids, MATS).astype(jnp.int32)
    holder = jnp.full((TOTAL_SLOTS,), -1, jnp.int32)
    return holder.at[ordering[:MATS]].set(identity)


def setup_inputs(seed: int = 0) -> dict:
    splits = jax.random.split(jax.random.key(seed), 4)
    grads = draw_grads(jax.random.fold_in(splits[3], 71), 0)
    momentum = draw_momentum(jax.random.fold_in(splits[3], 71), 0)
    slot_matrix = draw_slot_matrix(jax.random.fold_in(splits[3], 71), 0)
    return dict(grads=grads, momentum=momentum, slot_matrix=slot_matrix)


momentum_rate = 0.95
epsilon_norm = 1e-07
first_coef = 3.4445
third_coef = -4.775
fifth_coef = 2.0315

def orthogonal(initial):
    iterate = initial
    advanced = initial.astype(jnp.float32)
    for iteration in range(ITERS):
        gram_matrix = jnp.dot(iterate.T, iterate, preferred_element_type=jnp.float32).astype(jnp.bfloat16)
        square = jnp.dot(gram_matrix, gram_matrix, preferred_element_type=jnp.float32)
        polynomial = (third_coef * gram_matrix.astype(jnp.float32) + fifth_coef * square).astype(jnp.bfloat16)
        advanced = first_coef * iterate.astype(jnp.float32) + jnp.dot(iterate, polynomial, preferred_element_type=jnp.float32)
        if iteration + 1 < ITERS:
            iterate = advanced.astype(jnp.bfloat16)
    return (math.sqrt(C) * advanced).astype(jnp.bfloat16)

def reference(grads, momentum, slot_matrix):
    summed = lax.optimization_barrier(jnp.sum(grads, axis=0))
    present = (slot_matrix >= 0).astype(jnp.float32)
    picked = jnp.take(summed, jnp.maximum(slot_matrix, 0).astype(jnp.int32), axis=0) * present[:, None, None]
    renewed = momentum_rate * momentum + picked
    norms = jnp.sqrt(lax.optimization_barrier(jnp.sum(renewed * renewed, axis=(1, 2))))
    initial = (renewed / (norms + epsilon_norm)[:, None, None]).astype(jnp.bfloat16)
    matches = slot_matrix[None, :] == jnp.arange(MATS, dtype=jnp.int32)[:, None]
    slot_of = lax.optimization_barrier(jnp.sum(jnp.where(matches, jnp.arange(TOTAL_SLOTS, dtype=jnp.int32)[None, :], 0), axis=1)).astype(jnp.int32)
    chosen = jnp.take(initial, slot_of, axis=0)
    updates = lax.map(orthogonal, chosen)
    return (updates, renewed)
```

```python
import functools
import math

import jax
import jax.numpy as jnp
from jax import lax
from jax.experimental import pallas as pl
from jax.experimental.pallas import tpu as pltpu
from jax.sharding import PartitionSpec as P

ITERS = 5

momentum_rate = 0.95
epsilon_norm = 1e-07
first_coef = 3.4445
third_coef = -4.775
fifth_coef = 2.0315

MESH = pl.DeviceIdType.MESH
F32 = jnp.float32
BF16 = jnp.bfloat16


def low_bit(d):
    return (d & -d).bit_length() - 1


def poly_of(iterate):
    gram = lax.dot_general(
        iterate, iterate, (((0,), (0,)), ((), ())), preferred_element_type=F32
    ).astype(BF16)
    square = jnp.dot(gram, gram, preferred_element_type=F32)
    return (third_coef * gram.astype(F32) + fifth_coef * square).astype(BF16)


def kernel(
    n_dp, n_ow, per, workers, pieces,
    slots_ref, grads_ref, mom_ref, upd_ref, momout_ref,
    ypack, yrecv, zsend, zrecv, held, orecv, work, scale_ref, pall,
    ys, yr, zs, zr, os_, or_, ms, mr, as_, ar, pzs, pzr, pys, pyr, pxs, pxr, pcs, pcr,
):
    n_z = n_dp // 2
    n_x = n_ow // 2
    bits = n_z.bit_length() - 1
    mats = grads_ref.shape[0]
    rows = grads_ref.shape[1]
    cols = grads_ref.shape[2]
    full = n_ow * rows
    nb = mats // n_dp
    each = nb // pieces
    n_slots = mom_ref.shape[0]
    dp = lax.axis_index("dp")
    ow = lax.axis_index("owner")
    z = lax.div(dp, 2)
    y = lax.rem(dp, 2)
    x = lax.div(ow, 2)
    core = lax.rem(ow, 2)
    other = 2 * z + 1 - y
    sibling = 2 * x + 1 - core

    def flip(d):
        out = z
        for i in range(bits):
            if (d >> i) & 1:
                out = out + (1 << i) * (1 - 2 * lax.rem(lax.div(z, 1 << i), 2))
        return out

    def peer(i):
        return 2 * flip(1 << i) + y

    def member(d, s):
        return 2 * flip(d) + (y if s == 0 else 1 - y)

    def owner_at(t):
        return lax.rem(ow + t, n_ow)

    def owner_from(t):
        return lax.rem(ow - t + n_ow, n_ow)

    def remote(src, dst, send, recv, to):
        return pltpu.make_async_remote_copy(
            src_ref=src, dst_ref=dst, send_sem=send, recv_sem=recv,
            device_id=to, device_id_type=MESH,
        )

    sent = []

    def launch(copy, lane=None):
        when_worker(lane, copy.start)
        sent.append((copy, lane))
        return copy

    def when_worker(lane, fn):
        if lane is None or workers == n_ow:
            fn()
        else:
            pl.when(lane < workers)(fn)

    barrier = pltpu.get_barrier_semaphore()
    pl.semaphore_signal(barrier, inc=1, device_id=(other, ow), device_id_type=MESH)
    for i in range(bits):
        pl.semaphore_signal(barrier, inc=1, device_id=(peer(i), ow), device_id_type=MESH)
    for t in range(1, n_ow):
        pl.semaphore_signal(barrier, inc=1, device_id=(dp, owner_at(t)), device_id_type=MESH)

    held_slots = [slots_ref[dp * n_slots + k] for k in range(n_slots)]

    def partial(m):
        place = jnp.int32(0)
        weight = F32(0.0)
        for k in range(n_slots):
            hit = held_slots[k] == m
            place = jnp.where(hit, k, place)
            weight = jnp.where(hit, F32(momentum_rate), weight)
        return grads_ref[m] + weight * mom_ref[place]

    y_copies = {}
    for d in reversed(range(n_z)):
        for q in range(pieces):
            def pack(j, carry, d=d, q=q):
                b = q * each + j
                ypack[d, b] = partial(member(d, 1) * nb + b).astype(BF16)
                return carry
            lax.fori_loop(0, each, pack, 0)
            if d == n_z - 1 and q == 0:
                pl.semaphore_wait(barrier, 1 + bits + (n_ow - 1))
            part = pl.ds(q * each, each)
            y_copies[d, q] = launch(remote(
                ypack.at[d, part], yrecv.at[d, part], ys.at[d, q], yr.at[d, q], (other, ow)))

    def z_copy(d, q):
        part = pl.ds(q * each, each)
        return remote(
            zsend.at[d - 1, part], zrecv.at[d - 1, part], zs.at[d - 1, q], zr.at[d - 1, q],
            (peer(low_bit(d)), ow))

    for d in reversed(range(n_z)):
        steps = low_bit(d) if d else bits
        for q in range(pieces):
            y_copies[d, q].wait_recv()
            for i in range(steps):
                z_copy(d + (1 << i), q).wait_recv()

            def add(j, carry, d=d, q=q, steps=steps):
                b = q * each + j
                value = partial(member(d, 0) * nb + b) + yrecv[d, b].astype(F32)
                for i in range(steps):
                    value = value + zrecv[d + (1 << i) - 1, b].astype(F32)
                if d:
                    zsend[d - 1, b] = value.astype(BF16)
                else:
                    held[dp * nb + b] = value.astype(BF16)
                return carry
            lax.fori_loop(0, each, add, 0)
            if d:
                launch(z_copy(d, q))

    o_copies = []
    for t in range(1, n_ow):
        j = owner_at(t)
        copy = remote(
            held.at[pl.ds(dp * nb + j * per, per)], orecv.at[ow],
            os_.at[t - 1], or_.at[t - 1], (dp, j))
        launch(copy, j)
        o_copies.append(copy)

    def m_copy(d, q):
        where = pl.ds(member(d & (d - 1), 0) * nb + q * each, each)
        there = held.at[where]
        return remote(there, there, ms.at[d - 1, q], mr.at[d - 1, q], (peer(low_bit(d)), ow))

    def m_arrival(d, q):
        where = pl.ds(member(d, 0) * nb + q * each, each)
        here = held.at[where]
        return remote(here, here, ms.at[d - 1, q], mr.at[d - 1, q], (peer(low_bit(d)), ow))

    def across(d, q, s=0):
        where = pl.ds(member(d, s) * nb + q * each, each)
        piece = held.at[where]
        return remote(piece, piece, as_.at[d, q], ar.at[d, q], (other, ow))

    def m_spread(d, q):
        for i in reversed(range(low_bit(d) if d else bits)):
            launch(m_copy(d + (1 << i), q))
        launch(across(d, q))

    def m_pass(d):
        for q in range(pieces):
            m_arrival(d, q).wait_recv()
            m_spread(d, q)

    for q in range(pieces):
        m_spread(0, q)

    def begin():
        orecv[ow] = held[pl.ds(dp * nb + ow * per, per)]
        for copy in o_copies:
            copy.wait_recv()
        for p in range(per):
            block = jnp.concatenate([orecv[o, p].astype(F32) for o in range(n_ow)], axis=0)
            norm = jnp.sqrt(jnp.sum(block * block, axis=(0, 1), keepdims=True)) + epsilon_norm
            iterate = (block / norm).astype(BF16)
            scale_ref[p] = jnp.broadcast_to(math.sqrt(full) / norm, scale_ref.shape[1:])
            poly = poly_of(iterate)
            advanced = first_coef * iterate.astype(F32) + jnp.dot(
                iterate, poly, preferred_element_type=F32)
            work[p, pl.ds(0, full)] = advanced.astype(BF16)
            at_row = lax.broadcasted_iota(jnp.int32, (cols, cols), 0)
            at_col = lax.broadcasted_iota(jnp.int32, (cols, cols), 1)
            eye = jnp.where(at_row == at_col, F32(first_coef), F32(0.0))
            work[p, pl.ds(full, cols)] = (eye + poly.astype(F32)).astype(BF16)

    def sweeps(count):
        def run():
            for p in range(per):
                both = work[p]
                for _ in range(count):
                    poly = poly_of(both[:full])
                    both = (first_coef * both.astype(F32) + jnp.dot(
                        both, poly, preferred_element_type=F32)).astype(BF16)
                work[p] = both
        return run

    def end():
        for p in range(per):
            poly = poly_of(work[p, pl.ds(0, full)])
            factor = work[p, pl.ds(full, cols)]
            last = first_coef * factor.astype(F32) + jnp.dot(
                factor, poly, preferred_element_type=F32)
            pall[dp * nb + ow * per + p] = (scale_ref[p, 0:1] * last).astype(BF16)

    when_worker(ow, begin)
    when_worker(ow, sweeps(ITERS - 2))
    when_worker(ow, end)

    def unit(d, s, lane):
        return pall.at[pl.ds(member(d, s) * nb + lane * per, per)]

    def lane_from(t):
        return 2 * lax.rem(x - t + n_x, n_x) + core

    def lane_at(t):
        return 2 * lax.rem(x + t, n_x) + core

    def twin_from(t):
        return 2 * lax.rem(x - t + n_x, n_x) + 1 - core

    def pz_copy(d):
        there = unit(d & (d - 1), 0, ow)
        return remote(there, there, pzs.at[d - 1], pzr.at[d - 1], (peer(low_bit(d)), ow))

    def py_copy(d):
        there = unit(d, 0, ow)
        return remote(there, there, pys.at[d], pyr.at[d], (other, ow))

    def px_copy(d, s, t):
        there = unit(d, s, ow)
        return remote(there, there, pxs.at[t - 1, d, s], pxr.at[t - 1, d, s], (dp, lane_at(t)))

    def px_arrival(d, s, t):
        here = unit(d, s, lane_from(t))
        return remote(here, here, pxs.at[t - 1, d, s], pxr.at[t - 1, d, s], (dp, lane_at(t)))

    def pc_copy(d, s, t):
        there = unit(d, s, lane_from(t))
        return remote(there, there, pcs.at[t, d, s], pcr.at[t, d, s], (dp, sibling))

    def pc_arrival(d, s, t):
        here = unit(d, s, twin_from(t))
        return remote(here, here, pcs.at[t, d, s], pcr.at[t, d, s], (dp, sibling))

    def emit(d, s):
        for t in range(1, n_x):
            launch(px_copy(d, s, t), ow)
        launch(pc_copy(d, s, 0), ow)

    def p_spread(d):
        for i in reversed(range(low_bit(d) if d else bits)):
            launch(pz_copy(d + (1 << i)), ow)
        launch(py_copy(d), ow)
        emit(d, 0)

    def arrive_x(d, s):
        for t in range(1, n_x):
            lane = lane_from(t)
            when_worker(lane, px_arrival(d, s, t).wait_recv)
            launch(pc_copy(d, s, t), lane)

    def arrive_c(d, s):
        for t in range(n_x):
            when_worker(twin_from(t), pc_arrival(d, s, t).wait_recv)

    def form(d, s):
        first = member(d, s) * nb
        for b in range(nb):
            upd_ref[first + b] = jnp.dot(
                held[first + b], pall[first + b], preferred_element_type=F32).astype(BF16)

    def pz_arrival(d):
        here = unit(d, 0, ow)
        return remote(here, here, pzs.at[d - 1], pzr.at[d - 1], (peer(low_bit(d)), ow))

    def py_arrival(d):
        here = unit(d, 1, ow)
        return remote(here, here, pys.at[d], pyr.at[d], (other, ow))

    def renew():
        def one(k, carry):
            m = slots_ref[dp * n_slots + k]
            present = jnp.where(m >= 0, F32(1.0), F32(0.0))
            momout_ref[k] = present * held[jnp.maximum(m, 0)].astype(F32) + (
                1.0 - present) * (F32(momentum_rate) * mom_ref[k])
            return carry
        lax.fori_loop(0, n_slots, one, 0)

    order = [(0, 0), (0, 1)]
    for d in range(1, n_z):
        order.append((d, 0))
        if d > 1:
            order.append((d - 1, 1))
    order.append((n_z - 1, 1))
    lag_x, lag_c = 2, 4

    p_spread(0)
    for d in range(1, n_z - 1):
        m_pass(d)
    for i in range(len(order) + lag_c):
        if i < len(order):
            d, s = order[i]
            if s:
                when_worker(ow, py_arrival(d).wait_recv)
                emit(d, 1)
            elif d:
                when_worker(ow, pz_arrival(d).wait_recv)
                p_spread(d)
            if (d, s) == (n_z - 1, 0):
                m_pass(d)
        if 0 <= i - lag_x < len(order):
            arrive_x(*order[i - lag_x])
        if 0 <= i - lag_c < len(order):
            d, s = order[i - lag_c]
            arrive_c(d, s)
            if s:
                for q in range(pieces):
                    across(d, q, 1).wait_recv()
            form(d, s)
    renew()

    for copy, lane in sent:
        when_worker(lane, copy.wait_send)


def local(n_dp, n_ow, grads, momentum, slot_matrix):
    mats, rows, cols = grads.shape[1:]
    n_slots = momentum.shape[0]
    nb = mats // n_dp
    n_z = n_dp // 2
    n_x = n_ow // 2
    workers = min(nb, n_ow)
    per = nb // workers
    pieces = max(1, min(nb, 4 * nb // n_z))
    block = (rows, cols)
    vmem = pl.BlockSpec(memory_space=pltpu.VMEM)
    dma = pltpu.SemaphoreType.DMA
    hops = n_z - 1
    counts = (
        (n_z, pieces), (hops, pieces), (n_ow - 1,), (hops, pieces), (n_z, pieces),
        (hops,), (n_z,), (n_x - 1, n_z, 2), (n_x, n_z, 2),
    )
    sems = []
    for count in counts:
        sems += [dma(count)] * 2
    updates, renewed = pl.pallas_call(
        functools.partial(kernel, n_dp, n_ow, per, workers, pieces),
        out_shape=(
            jax.ShapeDtypeStruct((mats,) + block, BF16),
            jax.ShapeDtypeStruct(momentum.shape, F32),
        ),
        in_specs=[pl.BlockSpec(memory_space=pltpu.SMEM), vmem, vmem],
        out_specs=(vmem, vmem),
        scratch_shapes=[
            pltpu.VMEM((n_z, nb) + block, BF16),
            pltpu.VMEM((n_z, nb) + block, BF16),
            pltpu.VMEM((hops, nb) + block, BF16),
            pltpu.VMEM((hops, nb) + block, BF16),
            pltpu.VMEM((mats,) + block, BF16),
            pltpu.VMEM((n_ow, per) + block, BF16),
            pltpu.VMEM((per, n_ow * rows + cols, cols), BF16),
            pltpu.VMEM((per, 8, cols), F32),
            pltpu.VMEM((mats, cols, cols), BF16),
        ] + sems,
        compiler_params=pltpu.CompilerParams(collective_id=0, has_side_effects=True),
    )(slot_matrix, grads[0], momentum)
    return updates, renewed


def solution(mesh):
    return jax.shard_map(
        functools.partial(local, mesh.shape["dp"], mesh.shape["owner"]),
        mesh=mesh,
        in_specs=(P("dp", None, "owner", None), P("dp", "owner", None), P()),
        out_specs=(P(None, "owner", None), P("dp", "owner", None)),
        check_vma=False,
    )
```

```python
import functools
import math

import jax
import jax.numpy as jnp
from jax import lax
from jax.experimental import pallas as pl
from jax.experimental.pallas import tpu as pltpu
from jax.sharding import PartitionSpec as P

ITERS = 5

momentum_rate = 0.95
epsilon_norm = 1e-07
first_coef = 3.4445
third_coef = -4.775
fifth_coef = 2.0315

MESH = pl.DeviceIdType.MESH
F32 = jnp.float32
BF16 = jnp.bfloat16


def low_bit(d):
    return (d & -d).bit_length() - 1


def poly_of(iterate):
    gram = lax.dot_general(
        iterate, iterate, (((0,), (0,)), ((), ())), preferred_element_type=F32
    ).astype(BF16)
    square = jnp.dot(gram, gram, preferred_element_type=F32)
    return (third_coef * gram.astype(F32) + fifth_coef * square).astype(BF16)


def kernel(
    n_dp, n_ow, per, workers, pieces,
    slots_hbm, grads_hbm, mom_hbm, upd_ref, momout_ref,
    slots_ref, grads_ref, mom_ref, ypack, yrecv, zsend, zrecv, held, orecv, work, scale_ref, pall,
    slotss, gs, moms, ys, yr, zs, zr, os_, or_, ms, mr, as_, ar, pzs, pzr, pys, pyr, pxs, pxr, pcs, pcr,
):
    n_z = n_dp // 2
    n_x = n_ow // 2
    bits = n_z.bit_length() - 1
    mats = grads_ref.shape[0]
    rows = grads_ref.shape[1]
    cols = grads_ref.shape[2]
    full = n_ow * rows
    nb = mats // n_dp
    each = nb // pieces
    n_slots = mom_ref.shape[0]
    dp = lax.axis_index("dp")
    ow = lax.axis_index("owner")
    z = lax.div(dp, 2)
    y = lax.rem(dp, 2)
    x = lax.div(ow, 2)
    core = lax.rem(ow, 2)
    other = 2 * z + 1 - y
    sibling = 2 * x + 1 - core

    def flip(d):
        out = z
        for i in range(bits):
            if (d >> i) & 1:
                out = out + (1 << i) * (1 - 2 * lax.rem(lax.div(z, 1 << i), 2))
        return out

    def lane_from(t):
        return 2 * lax.rem(x - t + n_x, n_x) + core

    def lane_at(t):
        return 2 * lax.rem(x + t, n_x) + core

    def twin_from(t):
        return 2 * lax.rem(x - t + n_x, n_x) + 1 - core

    def member(d, s):
        return 2 * flip(d) + (y if s == 0 else 1 - y)

    def remote(src, dst, send, recv, to):
        return pltpu.make_async_remote_copy(
            src_ref=src, dst_ref=dst, send_sem=send, recv_sem=recv,
            device_id=to, device_id_type=MESH,
        )

    def only(cond, fn):
        if cond is None:
            fn()
        else:
            pl.when(cond)(fn)

    def works(lane):
        return None if workers == n_ow else lane < workers

    sent = []

    def launch(copy, cond=None):
        only(cond, copy.start)
        sent.append((copy, cond))

    barrier = pltpu.get_barrier_semaphore()

    def greet(member_id, lane):
        pl.semaphore_signal(barrier, inc=1, device_id=(member_id, lane), device_id_type=MESH)

    for d in range(1, n_z):
        greet(member(d, 0), ow)
    greet(other, ow)
    for t in range(1, n_ow):
        greet(dp, lax.rem(ow + t, n_ow))
    diagonal = tuple(range(FIRST_DIAG, n_z))
    for t in range(1, n_x if diagonal else 1):
        greet(other, lane_at(t))
    greeted = (n_z - 1) + 1 + (n_ow - 1) + (n_x - 1 if diagonal else 0)

    slots_copy = pltpu.make_async_copy(slots_hbm, slots_ref, slotss)
    slots_copy.start()
    mom_copy = pltpu.make_async_copy(mom_hbm, mom_ref, moms)
    mom_copy.start()

    def grads_copy(d, s):
        where = pl.ds(member(d, s) * nb, nb)
        return pltpu.make_async_copy(grads_hbm.at[where], grads_ref.at[where], gs.at[d, s])

    for s in (1, 0):
        for d in reversed(range(n_z)):
            grads_copy(d, s).start()

    slots_copy.wait()
    held_slots = [slots_ref[dp * n_slots + k] for k in range(n_slots)]

    def partial(m):
        place = jnp.int32(0)
        weight = F32(0.0)
        for k in range(n_slots):
            hit = held_slots[k] == m
            place = jnp.where(hit, k, place)
            weight = jnp.where(hit, F32(momentum_rate), weight)
        return grads_ref[m] + weight * mom_ref[place]

    mom_copy.wait()
    y_copies = {}
    for d in reversed(range(n_z)):
        grads_copy(d, 1).wait()
        for q in range(pieces):
            def pack(j, carry, d=d, q=q):
                b = q * each + j
                ypack[d, b] = partial(member(d, 1) * nb + b).astype(BF16)
                return carry
            lax.fori_loop(0, each, pack, 0)
            if d == n_z - 1 and q == 0:
                pl.semaphore_wait(barrier, greeted)
            part = pl.ds(q * each, each)
            y_copies[d, q] = remote(
                ypack.at[d, part], yrecv.at[d, part], ys.at[d, q], yr.at[d, q], (other, ow))
            launch(y_copies[d, q])
    for d in reversed(range(n_z)):
        grads_copy(d, 0).wait()

    def z_copy(d, q):
        part = pl.ds(q * each, each)
        return remote(
            zsend.at[d - 1, part], zrecv.at[d - 1, part], zs.at[d - 1, q], zr.at[d - 1, q],
            (member(1 << low_bit(d), 0), ow))

    def o_copy(b):
        return remote(
            held.at[pl.ds(dp * nb + b, 1)], orecv.at[ow, pl.ds(b % per, 1)],
            os_.at[b], or_.at[ow, b % per], (dp, b // per))

    def o_arrival(o, p):
        here = orecv.at[o, pl.ds(p, 1)]
        return remote(here, here, os_.at[p], or_.at[o, p], (dp, o))

    def m_copy(d, q):
        where = pl.ds(member(d & (d - 1), 0) * nb + q * each, each)
        there = held.at[where]
        return remote(
            there, there, ms.at[d - 1, q], mr.at[d - 1, q], (member(1 << low_bit(d), 0), ow))

    def m_arrival(d, q):
        where = pl.ds(member(d, 0) * nb + q * each, each)
        here = held.at[where]
        return remote(
            here, here, ms.at[d - 1, q], mr.at[d - 1, q], (member(1 << low_bit(d), 0), ow))

    def across(d, q, s=0):
        where = pl.ds(member(d, s) * nb + q * each, each)
        piece = held.at[where]
        return remote(piece, piece, as_.at[d, q], ar.at[d, q], (other, ow))

    def m_spread(d, q):
        for i in range(low_bit(d) if d else bits):
            launch(m_copy(d + (1 << i), q))
        launch(across(d, q))

    def m_pass(d, q):
        m_arrival(d, q).wait_recv()
        m_spread(d, q)

    for d in reversed(range(n_z)):
        steps = low_bit(d) if d else bits
        for q in range(pieces):
            y_copies[d, q].wait_recv()
            for i in range(steps):
                z_copy(d + (1 << i), q).wait_recv()

            def add(j, carry, d=d, q=q, steps=steps):
                b = q * each + j
                value = partial(member(d, 0) * nb + b) + yrecv[d, b].astype(F32)
                for i in range(steps):
                    value = value + zrecv[d + (1 << i) - 1, b].astype(F32)
                if d:
                    zsend[d - 1, b] = value.astype(BF16)
                else:
                    held[dp * nb + b] = value.astype(BF16)
                return carry
            lax.fori_loop(0, each, add, 0)
            if d:
                launch(z_copy(d, q))
            else:
                for b in range(q * each, (q + 1) * each):
                    launch(o_copy(b), ow != b // per)
                m_spread(0, q)

    passes = [(d, q) for d in range(1, n_z) for q in range(pieces)]

    def some(count):
        for _ in range(min(count, len(passes))):
            m_pass(*passes.pop(0))

    def begin():
        for p in range(per):
            orecv[ow, p] = held[dp * nb + ow * per + p]
            for o in range(n_ow):
                pl.when(ow != o)(o_arrival(o, p).wait_recv)
        for p in range(per):
            block = jnp.concatenate([orecv[o, p].astype(F32) for o in range(n_ow)], axis=0)
            norm = jnp.sqrt(jnp.sum(block * block, axis=(0, 1), keepdims=True)) + epsilon_norm
            iterate = (block / norm).astype(BF16)
            scale_ref[p] = jnp.broadcast_to(math.sqrt(full) / norm, scale_ref.shape[1:])
            poly = poly_of(iterate)
            advanced = first_coef * iterate.astype(F32) + jnp.dot(
                iterate, poly, preferred_element_type=F32)
            work[p, pl.ds(0, full)] = advanced.astype(BF16)
            at_row = lax.broadcasted_iota(jnp.int32, (cols, cols), 0)
            at_col = lax.broadcasted_iota(jnp.int32, (cols, cols), 1)
            eye = jnp.where(at_row == at_col, F32(first_coef), F32(0.0))
            work[p, pl.ds(full, cols)] = (eye + poly.astype(F32)).astype(BF16)

    def sweep():
        for p in range(per):
            both = work[p]
            poly = poly_of(both[:full])
            work[p] = (first_coef * both.astype(F32) + jnp.dot(
                both, poly, preferred_element_type=F32)).astype(BF16)

    def end():
        for p in range(per):
            poly = poly_of(work[p, pl.ds(0, full)])
            factor = work[p, pl.ds(full, cols)]
            last = first_coef * factor.astype(F32) + jnp.dot(
                factor, poly, preferred_element_type=F32)
            pall[dp * nb + ow * per + p] = (scale_ref[p, 0:1] * last).astype(BF16)

    some(PRE)
    only(works(ow), begin)
    for _ in range(ITERS - 2):
        some(MID)
        only(works(ow), sweep)
    some(MID)
    only(works(ow), end)

    def unit(d, s, lane):
        return pall.at[pl.ds(member(d, s) * nb + lane * per, per)]

    def pz_copy(d, arrival=False):
        there = unit(d if arrival else 0, 0, ow)
        return remote(there, there, pzs.at[d - 1], pzr.at[d - 1], (member(d, 0), ow))

    def py_copy(d, s=0):
        there = unit(d, s, ow)
        return remote(there, there, pys.at[d], pyr.at[d], (other, ow))

    def px_copy(d, s, t, arrival=False):
        there = unit(d, s, lane_from(t) if arrival else ow)
        return remote(there, there, pxs.at[t - 1, d, s], pxr.at[t - 1, d, s], (dp, lane_at(t)))

    def pc_copy(d, s, t, arrival=False):
        there = unit(d, s, twin_from(t) if arrival else lane_from(t))
        return remote(there, there, pcs.at[t, d, s], pcr.at[t, d, s], (dp, sibling))

    def pd_copy(d, t, arrival=False):
        there = unit(d, 1 if arrival else 0, lane_from(t) if arrival else ow)
        return remote(
            there, there, pxs.at[t - 1, d, 1], pxr.at[t - 1, d, 1], (other, lane_at(t)))

    def emit(d, s):
        for t in range(1, n_x):
            if not (s and d in diagonal):
                launch(px_copy(d, s, t), works(ow))
            if not s and d in diagonal:
                launch(pd_copy(d, t), works(ow))
        launch(pc_copy(d, s, 0), works(ow))

    def at_y(d):
        only(works(ow), py_copy(d, 1).wait_recv)
        emit(d, 1)

    def at_z(d):
        only(works(ow), pz_copy(d, True).wait_recv)
        launch(py_copy(d), works(ow))
        emit(d, 0)

    def at_x(d, s):
        for t in range(1, n_x):
            lane = lane_from(t)
            arrived = pd_copy(d, t, True) if s and d in diagonal else px_copy(d, s, t, True)
            only(works(lane), arrived.wait_recv)
            launch(pc_copy(d, s, t), works(lane))

    landed = set()

    def far_rows(d):
        if d not in landed:
            landed.add(d)
            for q in range(pieces):
                across(d, q, 1).wait_recv()

    def form(d, s):
        for t in range(n_x):
            only(works(twin_from(t)), pc_copy(d, s, t, True).wait_recv)
        if s:
            far_rows(d)
        first = member(d, s) * nb
        for b in range(nb):
            upd_ref[first + b] = jnp.dot(
                held[first + b], pall[first + b], preferred_element_type=F32).astype(BF16)

    def renew():
        for d in range(n_z):
            far_rows(d)

        def one(k, carry):
            m = slots_ref[dp * n_slots + k]
            present = jnp.where(m >= 0, F32(1.0), F32(0.0))
            momout_ref[k] = present * held[jnp.maximum(m, 0)].astype(F32) + (
                1.0 - present) * (F32(momentum_rate) * mom_ref[k])
            return carry
        lax.fori_loop(0, n_slots, one, 0)

    for d in reversed(range(1, n_z)):
        launch(pz_copy(d), works(ow))
    launch(py_copy(0), works(ow))
    emit(0, 0)
    some(len(passes) - LATE * pieces)
    at_y(0)
    at_x(0, 0)
    for d in range(1, n_z):
        at_z(d)
    some(len(passes))
    at_x(0, 1)
    formed = [(0, 0), (0, 1)] + [(d, 0) for d in range(1, n_z)] + [(d, 1) for d in range(1, n_z)]
    for d in range(1, n_z):
        at_y(d)
        at_x(d, 0)
        form(*formed.pop(0))
    for d in range(1, n_z):
        form(*formed.pop(0))
        if d == n_z - 1:
            renew()
        at_x(d, 1)
    while formed:
        form(*formed.pop(0))

    for copy, cond in sent:
        only(cond, copy.wait_send)


def writer(upd_ref, mom_ref, upd_hbm, mom_hbm, sems):
    parts = sems.shape[0] // 2
    copies = []
    for i, (src, dst) in enumerate(((upd_ref, upd_hbm), (mom_ref, mom_hbm))):
        count = src.shape[0] // parts
        for q in range(parts):
            where = pl.ds(q * count, count)
            copies.append(pltpu.make_async_copy(src.at[where], dst.at[where], sems.at[i * parts + q]))
    for copy in copies:
        copy.start()
    for copy in copies:
        copy.wait()


PRE, MID, LATE = 2, 1, 1
FIRST_DIAG = 99


def local(n_dp, n_ow, grads, momentum, slot_matrix):
    mats, rows, cols = grads.shape[1:]
    n_slots = momentum.shape[0]
    nb = mats // n_dp
    n_z = n_dp // 2
    n_x = n_ow // 2
    workers = min(nb, n_ow)
    per = nb // workers
    pieces = max(1, min(nb, 4 * nb // n_z))
    block = (rows, cols)
    vmem = pl.BlockSpec(memory_space=pltpu.VMEM)
    hbm = pl.BlockSpec(memory_space=pltpu.HBM)
    dma = pltpu.SemaphoreType.DMA
    hops = n_z - 1
    counts = (
        (n_z, pieces), (hops, pieces), None, (hops, pieces), (n_z, pieces),
        (hops,), (n_z,), (n_x - 1, n_z, 2), (n_x, n_z, 2),
    )
    sems = [dma, dma((n_z, 2)), dma]
    for count in counts:
        sems += [dma(count)] * 2 if count else [dma((nb,)), dma((n_ow, per))]
    own_grads = pltpu.with_memory_space_constraint(grads[0], pltpu.HBM)
    own_slots = pltpu.with_memory_space_constraint(slot_matrix, pltpu.HBM)
    own_momentum = pltpu.with_memory_space_constraint(momentum, pltpu.HBM)
    updates, renewed = pl.pallas_call(
        functools.partial(kernel, n_dp, n_ow, per, workers, pieces),
        out_shape=(
            pltpu.VMEM((mats,) + block, BF16),
            pltpu.VMEM(momentum.shape, F32),
        ),
        in_specs=[hbm, hbm, hbm],
        out_specs=(vmem, vmem),
        scratch_shapes=[
            pltpu.SMEM(slot_matrix.shape, jnp.int32),
            pltpu.VMEM((mats,) + block, F32),
            pltpu.VMEM((n_slots,) + block, F32),
            pltpu.VMEM((n_z, nb) + block, BF16),
            pltpu.VMEM((n_z, nb) + block, BF16),
            pltpu.VMEM((hops, nb) + block, BF16),
            pltpu.VMEM((hops, nb) + block, BF16),
            pltpu.VMEM((mats,) + block, BF16),
            pltpu.VMEM((n_ow, per) + block, BF16),
            pltpu.VMEM((per, n_ow * rows + cols, cols), BF16),
            pltpu.VMEM((per, 8, cols), F32),
            pltpu.VMEM((mats, cols, cols), BF16),
        ] + sems,
        compiler_params=pltpu.CompilerParams(
            collective_id=0, has_side_effects=True, vmem_limit_bytes=40 * 2**20),
    )(own_slots, own_grads, own_momentum)
    return pl.pallas_call(
        writer,
        out_shape=(
            jax.ShapeDtypeStruct((mats,) + block, BF16),
            jax.ShapeDtypeStruct(momentum.shape, F32),
        ),
        in_specs=[vmem, vmem],
        out_specs=(hbm, hbm),
        scratch_shapes=[dma((8,))],
        compiler_params=pltpu.CompilerParams(vmem_limit_bytes=40 * 2**20),
    )(updates, renewed)


def solution(mesh):
    return jax.shard_map(
        functools.partial(local, mesh.shape["dp"], mesh.shape["owner"]),
        mesh=mesh,
        in_specs=(P("dp", None, "owner", None), P("dp", "owner", None), P()),
        out_specs=(P(None, "owner", None), P("dp", "owner", None)),
        check_vma=False,
    )
```
